64 devices in a mesh: dp: 4 (over x, y), vp: 16 (over z, core).
Axes of the slice: x: 2, y: 2, z: 8, core: 2. Of those that a mesh axis runs over, the one named last changes fastest.
The devices are a block of a 4x4x8 slice.
Arguments:
- hidden: bfloat16 [256, 128, 768], P('vp', 'dp'), parts along dimension 1
- norm_gain: float32 [768], replicated
- norm_bias: float32 [768], replicated
- w_out: bfloat16 [768, 51200], P(None, 'vp')
- labels: int32 [256, 128], P('vp', 'dp'), parts along dimension 1
- loss_mask: float32 [256, 128], P('vp', 'dp'), parts along dimension 1
Outputs:
- output 1: float32 [4], P('dp'), parts along dimension 0
- output 2: bfloat16 [256, 128, 768], P('vp', 'dp'), parts along dimension 1
- output 3: float32 [3072, 51200], P('dp', 'vp'), parts along dimension 0
- output 4: float32 [3072], P('dp'), parts along dimension 0
- output 5: float32 [3072], P('dp'), parts along dimension 0
There are 4 independent parts. The reference program is written for one: setup_inputs(seed, part) draws one part's arguments, and reference() takes and returns one part's arrays. A program takes and returns all parts, laid end to end along the dimension named above; an argument that names none is the same for every part.
All inputs are finite; a program needn't handle non-finite values.
Results may differ from the reference program's by a relative error of at most 0.001.
Values are sent between devices in bfloat16 or wider.
A program may use at most 768 MiB of HBM per device.

```python
import jax
import jax.numpy as jnp
from jax import lax

SEQ_DEV = 16
GROUP_SIZE = 16
BATCH_PART = 32
D_MODEL = 768
VOCAB_SIZE = 50304
VOCAB_PAD = 51200
NORM_EPS = 1e-5
SEQ_LEN = SEQ_DEV * GROUP_SIZE
BLOCK_TOKENS = SEQ_DEV * BATCH_PART


def draw_labels(rng_key):
    key_pick, key_flat, key_upper, key_inner, key_skew = jax.random.split(rng_key, 5)
    tok_shape = (SEQ_LEN, BATCH_PART)
    flat_ids = jax.random.randint(key_flat, tok_shape, 0, VOCAB_SIZE)
    upper_one = jax.random.randint(key_upper, tok_shape, 1, VOCAB_SIZE + 1)
    upper_two = jax.random.randint(key_inner, tok_shape, 1, upper_one + 1)
    skew_ids = jax.random.randint(key_skew, tok_shape, 0, upper_two)
    pick_flat = jax.random.randint(key_pick, tok_shape, 0, 2)
    label_ids = jnp.where(pick_flat == 0, flat_ids, skew_ids)
    label_ids = label_ids.at[0, 0].set(VOCAB_SIZE - 1)
    return label_ids.at[SEQ_LEN - 1, BATCH_PART - 1].set(0)


def draw_mask(rng_key):
    mask_ids = jax.random.randint(rng_key, (SEQ_LEN, BATCH_PART), 0, 4)
    return (mask_ids > 0).astype(jnp.float32).at[0, 0].set(1.0)


def setup_inputs(seed: int = 0, part: int = 0) -> dict:
    root_key = jax.random.key(seed)
    shared_key, part_base = jax.random.split(root_key)
    part_key = jax.random.fold_in(part_base, part)
    key_w, key_g, key_c = jax.random.split(shared_key, 3)
    key_x, key_lab, key_mask = jax.random.split(part_key, 3)
    hidden = jax.random.normal(key_x, (SEQ_LEN, BATCH_PART, D_MODEL), jnp.float32).astype(jnp.bfloat16)
    norm_gain = 0.3 * jax.random.normal(key_g, (D_MODEL,), jnp.float32)
    norm_bias = 0.5 * jax.random.normal(key_c, (D_MODEL,), jnp.float32)
    w_out = (jax.random.normal(key_w, (D_MODEL, VOCAB_PAD), jnp.float32) * (2.0 / D_MODEL ** 0.5)).astype(jnp.bfloat16)
    labels = draw_labels(key_lab)
    loss_mask = draw_mask(key_mask)
    return {"hidden": hidden, "norm_gain": norm_gain, "norm_bias": norm_bias, "w_out": w_out, "labels": labels, "loss_mask": loss_mask}


def reference(hidden, norm_gain, norm_bias, w_out, labels, loss_mask):
    mask_total = jnp.sum(loss_mask)
    x_blocks = hidden.reshape(GROUP_SIZE, BLOCK_TOKENS, D_MODEL)
    lab_blocks = labels.reshape(GROUP_SIZE, BLOCK_TOKENS)
    mask_blocks = loss_mask.reshape(GROUP_SIZE, BLOCK_TOKENS)
    col_ids = jnp.arange(VOCAB_PAD, dtype=jnp.int32)

    def block_step(acc_state, block_in):
        grad_w, loss_sum, gain_sum, bias_sum = acc_state
        x_blk, lab_blk, mask_blk = block_in
        x_float = x_blk.astype(jnp.float32)
        tok_mean = jnp.mean(x_float, axis=-1, keepdims=True)
        centered = x_float - tok_mean
        inv_std = lax.rsqrt(jnp.mean(centered * centered, axis=-1, keepdims=True) + NORM_EPS)
        normed = centered * inv_std
        h_blk = (normed * (1.0 + norm_gain) + norm_bias).astype(jnp.bfloat16)
        logits = jnp.dot(h_blk, w_out, preferred_element_type=jnp.float32)
        row_max = jnp.max(logits, axis=-1, keepdims=True)
        exp_shift = jnp.exp(logits - row_max)
        sum_exp = jnp.sum(exp_shift, axis=-1, keepdims=True)
        is_label = (col_ids[None, :] == lab_blk[:, None]).astype(jnp.float32)
        target = jnp.sum(logits * is_label, axis=-1)
        tok_loss = row_max[:, 0] + jnp.log(sum_exp[:, 0]) - target
        tok_weight = mask_blk / mask_total
        grad_logits = ((exp_shift / sum_exp - is_label) * tok_weight[:, None]).astype(jnp.bfloat16)
        grad_w = grad_w + jnp.dot(h_blk.T, grad_logits, preferred_element_type=jnp.float32)
        grad_h = jnp.dot(grad_logits, w_out.T, preferred_element_type=jnp.float32)
        gain_sum = gain_sum + jnp.sum(grad_h * normed, axis=0)
        bias_sum = bias_sum + jnp.sum(grad_h, axis=0)
        scaled = grad_h * (1.0 + norm_gain)
        grad_x = inv_std * (scaled - jnp.mean(scaled, axis=-1, keepdims=True) - normed * jnp.mean(scaled * normed, axis=-1, keepdims=True))
        loss_sum = loss_sum + jnp.sum(mask_blk * tok_loss)
        return (grad_w, loss_sum, gain_sum, bias_sum), grad_x.astype(jnp.bfloat16)

    init_state = (jnp.zeros((D_MODEL, VOCAB_PAD), jnp.float32), jnp.zeros((), jnp.float32), jnp.zeros((D_MODEL,), jnp.float32), jnp.zeros((D_MODEL,), jnp.float32))
    final_state, grad_x = lax.scan(block_step, init_state, (x_blocks, lab_blocks, mask_blocks))
    grad_w, loss_sum, gain_sum, bias_sum = final_state
    loss = (loss_sum / mask_total).reshape(1)
    return loss, grad_x.reshape(SEQ_LEN, BATCH_PART, D_MODEL), grad_w, gain_sum, bias_sum
```

```python
import functools

import jax
import jax.numpy as jnp
from jax import lax
from jax.experimental import pallas as pl
from jax.experimental.pallas import tpu as pltpu
from jax.sharding import PartitionSpec as P

NORM_EPS = 1e-5
F32 = jnp.float32
BF16 = jnp.bfloat16
MESH = pl.DeviceIdType.MESH


def row_chunk(rows, limit):
    best = 16
    for size in range(16, limit + 1, 16):
        if rows % size == 0:
            best = size
    return best


def head_kernel(
    n, x_ref, gain_ref, bias_ref, w_hbm, aux_ref,
    dx_ref, dwt_hbm, dgain_ref, dbias_ref, loss_ref, z_hbm,
    w_v, wt, h_all, dw_acc, zbuf, dzb, h_pair, own, give, ring_in, mate_in,
    aux_all, st_loc, st_all, lse_all, t_acc, fin_all,
    w_sem, dw_sem, z_sem,
    f_send, f_recv, p_send, p_recv,
    a_send, a_recv, s_send, s_recv, l_send, l_recv, e_send, e_recv,
    r_send, r_recv, q_send, q_recv, r_cred, q_cred,
):
    chips = n // 2
    me = lax.axis_index("vp")
    zc, core = me // 2, me % 2
    mate = zc * 2 + 1 - core
    up = lax.rem(zc + 1, chips) * 2 + core
    down = lax.rem(zc + chips - 1, chips) * 2 + core
    ahead = (up, down)
    depth, cols = w_v.shape
    half = x_ref.shape[0] // 2
    sub = half // 2
    vchunk = row_chunk(cols, 640)
    col_start = me * cols

    def remote(src, dst, send, recv, dev):
        return pltpu.make_async_remote_copy(
            src_ref=src, dst_ref=dst, send_sem=send, recv_sem=recv,
            device_id={"vp": dev}, device_id_type=MESH)

    def peer_of(k):
        return lax.rem(me + k, n)

    w_copy = pltpu.make_async_copy(w_hbm, w_v, w_sem)
    w_copy.start()

    barrier = pltpu.get_barrier_semaphore()
    for k in range(1, n):
        pl.semaphore_signal(barrier, inc=1, device_id={"vp": peer_of(k)}, device_id_type=MESH)

    gain = 1.0 + gain_ref[...]
    bias = bias_ref[...]

    def normed_rows(rows):
        xf = rows.astype(F32)
        centered = xf - jnp.mean(xf, axis=-1, keepdims=True)
        inv_std = lax.rsqrt(jnp.mean(centered * centered, axis=-1, keepdims=True) + NORM_EPS)
        return centered * inv_std, inv_std

    ln_rows = half // 4

    @pl.loop(0, 8)
    def _(i):
        row0 = pl.multiple_of((i % 4) * ln_rows, ln_rows)
        src0 = pl.multiple_of(i * ln_rows, ln_rows)
        normed, _ = normed_rows(x_ref[pl.ds(src0, ln_rows), :])
        h_all[me, i // 4, pl.ds(row0, ln_rows), :] = (normed * gain + bias).astype(BF16)

    aux_all[me] = aux_ref[...]
    t_acc[...] = jnp.zeros_like(t_acc)
    pl.semaphore_wait(barrier, n - 1)

    def ring_copy(d, k, blk, hf):
        ref = h_all.at[blk, hf]
        return remote(ref, ref, f_send.at[d, k], f_recv.at[d, k], ahead[d])

    def mate_copy(d, k, blk, hf):
        ref = h_all.at[blk, hf]
        return remote(ref, ref, p_send.at[d, k], p_recv.at[d, k], mate)

    def fwd_half(d, k):
        return (k + 1) % 2 if d == 0 else k % 2

    for k in (1, 2):
        for d in (0, 1):
            ring_copy(d, k, me, fwd_half(d, k)).start()

    def spread(ref, dst, send, recv):
        for k in range(1, n):
            remote(ref, dst, send.at[k], recv.at[me], peer_of(k)).start()

    def collect(ref_all, send, recv):
        for k in range(1, n):
            src = peer_of(k)
            remote(ref_all.at[src], ref_all.at[src], send.at[k], recv.at[src], src).wait_recv()

    def drain(ref, send, recv):
        for k in range(1, n):
            remote(ref, ref, send.at[k], recv.at[me], peer_of(k)).wait_send()

    spread(aux_all.at[me], aux_all.at[me], a_send, a_recv)

    w_copy.wait()
    tcols = 128 if cols % 128 == 0 else cols

    @pl.loop(0, cols // tcols)
    def _(i):
        c0 = pl.multiple_of(i * tcols, tcols)
        wt[pl.ds(c0, tcols), :] = w_v[:, pl.ds(c0, tcols)].T

    @pl.loop(0, cols // vchunk)
    def _(i):
        c0 = pl.multiple_of(i * vchunk, vchunk)
        dw_acc[pl.ds(c0, vchunk), :] = jnp.zeros((vchunk, depth), F32)

    last = chips - 1

    def z_out(slot, tile):
        return pltpu.make_async_copy(zbuf.at[slot], z_hbm.at[tile], z_sem.at[slot])

    def fwd_chip(d, k):
        step = (k + 1) // 2
        return lax.rem(zc + chips - step, chips) if d == 0 else lax.rem(zc + step, chips)

    @pl.loop(0, chips)
    def _(k):
        for d in (0, 1):
            blk = fwd_chip(d, k) * 2 + core
            hf = fwd_half(d, k)

            @pl.when(k >= 1)
            def _():
                ring_copy(d, k, blk, hf).wait_recv()

                @pl.when(k + 2 <= last)
                def _():
                    ring_copy(d, k + 2, blk, hf).start()

            mate_copy(d, k, blk, hf).start()

        @pl.loop(0, 4)
        def _(q):
            d = q % 2
            step = (k + 1) // 2
            chip = lax.rem(zc + 2 * chips + (2 * d - 1) * step, chips)
            hf = lax.rem(k + 1 + d, 2)
            blk = chip * 2 + jnp.where(q < 2, core, 1 - core)

            @pl.when(q >= 2)
            def _():
                mate_copy(d, k, blk, hf).wait_recv()

            slot = d

            @pl.when(k * 4 + q >= 2)
            def _():
                z_out(slot, 0).wait()

            m8 = jnp.full((8, half), -jnp.inf, F32)
            s8 = jnp.zeros((8, half), F32)
            h_tile = h_all[blk, hf]
            for j in range(cols // vchunk):
                rows = pl.ds(j * vchunk, vchunk)
                z = lax.dot_general(wt[rows, :], h_tile, (((1,), (1,)), ((), ())), preferred_element_type=F32)
                zbuf[slot, rows, :] = z
                z3 = z.reshape(vchunk // 8, 8, half)
                m_new = jnp.maximum(m8, jnp.max(z3, axis=0))
                s8 = s8 * jnp.exp(m8 - m_new) + jnp.sum(jnp.exp(z3 - m_new[None]), axis=0)
                m8 = m_new
            m1 = jnp.max(m8, axis=0, keepdims=True)
            st_loc[blk, hf, 0:1, :] = m1
            st_loc[blk, hf, 1:2, :] = jnp.sum(s8 * jnp.exp(m8 - m1), axis=0, keepdims=True)
            z_out(slot, blk * 2 + hf).start()

    z_out(0, 0).wait()
    z_out(1, 0).wait()

    def bwd_place(j):
        d, s = lax.rem(j, 2), j // 2
        chip = lax.rem(zc + 2 * chips + (2 * d - 1) * (s + 1), chips)
        return d, s, chip

    def z_in(slot, j):
        d, _, chip = bwd_place(j)
        blk = chip * 2 + (core if slot == 0 else 1 - core)
        return pltpu.make_async_copy(z_hbm.at[blk * 2 + d], zbuf.at[slot], z_sem.at[slot])

    z_in(0, 0).start()
    z_in(1, 0).start()

    for k in range(1, n):
        peer = peer_of(k)
        remote(st_loc.at[peer], st_all.at[me], s_send.at[k], s_recv.at[me], peer).start()
    st_all[me] = st_loc[me]
    collect(st_all, s_send, s_recv)
    for hf in (0, 1):
        tops = [st_all[i, hf, 0:1, :] for i in range(n)]
        top = functools.reduce(jnp.maximum, tops)
        total = functools.reduce(jnp.add, [st_all[i, hf, 1:2, :] * jnp.exp(tops[i] - top) for i in range(n)])
        lse_all[me, hf] = top + jnp.log(total)
    spread(lse_all.at[me], lse_all.at[me], l_send, l_recv)
    collect(aux_all, a_send, a_recv)
    mask_sum = functools.reduce(jnp.add, [aux_all[i, hf, 1:2, :] for i in range(n) for hf in (0, 1)])
    mask_total = jnp.sum(mask_sum, axis=1, keepdims=True)
    collect(lse_all, l_send, l_recv)

    def ring_sum(d, slot, sb):
        return remote(own.at[d, slot, sb], ring_in.at[d, slot, sb], r_send.at[d, slot, sb], r_recv.at[d, slot, sb],
                      jnp.where(d == 0, up, down))

    def mate_sum(d, slot):
        return remote(give.at[d, slot], mate_in.at[d, slot], q_send.at[d, slot], q_recv.at[d, slot], mate)

    def event(j, sb):
        d, s, _ = bwd_place(j)
        slot = lax.rem(s, 2)
        prev = lax.rem(s + 1, 2)
        if sb == 0:
            mate_sum(d, slot).wait_recv()

        @pl.when(s == 0)
        def _():
            own[d, slot, sb] = own[d, slot, sb] + mate_in[d, slot, sb]

        @pl.when(s >= 1)
        def _():
            ring_sum(d, prev, sb).wait_recv()
            own[d, slot, sb] = (own[d, slot, sb] + mate_in[d, slot, sb]) + ring_in[d, prev, sb]

        @pl.when(s <= chips - 2)
        def _():
            if sb == 0:
                @pl.when(s >= 2)
                def _():
                    pl.semaphore_wait(r_cred.at[d], 1)
            ring_sum(d, slot, sb).start()

        if sb == 1:
            @pl.when((s >= 1) & (s <= chips - 3))
            def _():
                pl.semaphore_signal(r_cred.at[d], inc=1, device_id={"vp": jnp.where(d == 0, down, up)}, device_id_type=MESH)

            @pl.when(s <= chips - 3)
            def _():
                pl.semaphore_signal(q_cred.at[d], inc=1, device_id={"vp": mate}, device_id_type=MESH)

    pairs = 2 * chips

    @pl.loop(0, pairs)
    def _(j):
        d, s, chip = bwd_place(j)
        slot = lax.rem(s, 2)
        blks = (chip * 2 + core, chip * 2 + 1 - core)
        for side in (0, 1):
            blk = blks[side]
            lanes = pl.ds(side * half, half)
            lab = aux_all[blk, d, 0:1, :].astype(jnp.int32) - col_start
            mask = aux_all[blk, d, 1:2, :]
            weight = mask / mask_total
            lse = lse_all[blk, d]
            h_pair[pl.ds(side * half, half), :] = h_all[blk, d]
            z_in(side, j).wait()
            t8 = jnp.zeros((8, half), F32)
            for i in range(cols // vchunk):
                rows = pl.ds(i * vchunk, vchunk)
                z = zbuf[side, rows, :]
                hit = lax.broadcasted_iota(jnp.int32, (vchunk, half), 0) + i * vchunk == lab
                prob = jnp.exp(z - lse)
                dzb[rows, lanes] = (jnp.where(hit, prob - 1.0, prob) * weight).astype(BF16)
                t8 = t8 + jnp.sum(jnp.where(hit, z, 0.0).reshape(vchunk // 8, 8, half), axis=0)
            t_acc[...] += t8 * mask

            @pl.when(j + 1 < pairs)
            def _():
                z_in(side, j + 1).start()

        @pl.when(s >= 2)
        def _():
            mate_sum(d, slot).wait_send()
            for sb in (0, 1):
                ring_sum(d, slot, sb).wait_send()

        def partial(side, dst):
            g = jnp.dot(w_v[...], dzb[:, pl.ds(side * half, half)], preferred_element_type=F32)
            for sb in (0, 1):
                dst[d, slot, sb] = g[:, sb * sub:(sb + 1) * sub]

        partial(1, give)

        @pl.when(s >= 2)
        def _():
            pl.semaphore_wait(q_cred.at[d], 1)
        mate_sum(d, slot).start()
        partial(0, own)

        @pl.loop(0, cols // vchunk)
        def _(i):
            r0 = pl.multiple_of(i * vchunk, vchunk)
            rows = pl.ds(r0, vchunk)
            dw_acc[rows, :] += jnp.dot(dzb[rows, :], h_pair[...], preferred_element_type=F32)

        event(j, 0)

        @pl.when(j >= 1)
        def _():
            event(j - 1, 1)

    dw_copy = pltpu.make_async_copy(dw_acc, dwt_hbm, dw_sem)
    dw_copy.start()
    event(pairs - 1, 1)

    last_slot = (chips - 1) % 2
    dg = jnp.zeros((1, depth), F32)
    dc = jnp.zeros((1, depth), F32)
    for hf in (0, 1):
        for sb in (0, 1):
            rows = pl.ds(hf * half + sb * sub, sub)
            dh = own[hf, last_slot, sb].T
            normed, inv_std = normed_rows(x_ref[rows, :])
            dg = dg + jnp.sum(dh * normed, axis=0, keepdims=True)
            dc = dc + jnp.sum(dh, axis=0, keepdims=True)
            scaled = dh * gain
            mean_q = jnp.mean(scaled, axis=-1, keepdims=True)
            mean_qn = jnp.mean(scaled * normed, axis=-1, keepdims=True)
            dx_ref[rows, :] = (inv_std * (scaled - mean_q - normed * mean_qn)).astype(BF16)
    fin_all[me, 0:1, :] = dg
    fin_all[me, 1:2, :] = dc
    t_here = jnp.sum(jnp.sum(t_acc[...], axis=0, keepdims=True), axis=1, keepdims=True)
    fin_all[me, 2:3, :] = jnp.broadcast_to(t_here, (1, depth))
    fin_all[me, 3:4, :] = jnp.zeros((1, depth), F32)
    spread(fin_all.at[me], fin_all.at[me], e_send, e_recv)
    lse_sum = functools.reduce(
        jnp.add, [aux_all[i, hf, 1:2, :] * lse_all[i, hf] for i in range(n) for hf in (0, 1)])
    lse_total = jnp.sum(lse_sum, axis=1, keepdims=True)
    collect(fin_all, e_send, e_recv)
    dgain_ref[...] = functools.reduce(jnp.add, [fin_all[i, 0:1, :] for i in range(n)])
    dbias_ref[...] = functools.reduce(jnp.add, [fin_all[i, 1:2, :] for i in range(n)])
    t_total = functools.reduce(jnp.add, [fin_all[i, 2:3, 0:128] for i in range(n)])
    loss_ref[...] = (lse_total - t_total) / mask_total

    for k in range(1, chips):
        for d in (0, 1):
            ring_copy(d, k, me, 0).wait_send()
    for k in range(chips):
        for d in (0, 1):
            mate_copy(d, k, me, 0).wait_send()
    drain(aux_all.at[me], a_send, a_recv)
    drain(st_loc.at[me], s_send, s_recv)
    drain(lse_all.at[me], l_send, l_recv)
    drain(fin_all.at[me], e_send, e_recv)
    for d in (0, 1):
        for sb in (0, 1):
            ring_sum(d, (chips - 2) % 2, sb).wait_send()
        for slot in (0, 1):
            mate_sum(d, slot).wait_send()
    dw_copy.wait()


def head_call(n, x, gain, bias, w, aux):
    tokens, depth = x.shape
    cols = w.shape[1]
    half = tokens // 2
    sub = half // 2
    chips = n // 2
    vmem = pl.BlockSpec(memory_space=pltpu.VMEM)
    anywhere = pl.BlockSpec(memory_space=pl.ANY)
    dma = pltpu.SemaphoreType.DMA
    return pl.pallas_call(
        functools.partial(head_kernel, n),
        out_shape=(
            jax.ShapeDtypeStruct((tokens, depth), BF16),
            jax.ShapeDtypeStruct((cols, depth), F32),
            jax.ShapeDtypeStruct((1, depth), F32),
            jax.ShapeDtypeStruct((1, depth), F32),
            jax.ShapeDtypeStruct((1, 128), F32),
            jax.ShapeDtypeStruct((2 * n, cols, half), F32),
        ),
        in_specs=[vmem, vmem, vmem, anywhere, vmem],
        out_specs=(vmem, anywhere, vmem, vmem, vmem, anywhere),
        scratch_shapes=[
            pltpu.VMEM((depth, cols), BF16),
            pltpu.VMEM((cols, depth), BF16),
            pltpu.VMEM((n, 2, half, depth), BF16),
            pltpu.VMEM((cols, depth), F32),
            pltpu.VMEM((2, cols, half), F32),
            pltpu.VMEM((cols, tokens), BF16),
            pltpu.VMEM((tokens, depth), BF16),
            pltpu.VMEM((2, 2, 2, depth, sub), F32),
            pltpu.VMEM((2, 2, 2, depth, sub), F32),
            pltpu.VMEM((2, 2, 2, depth, sub), F32),
            pltpu.VMEM((2, 2, 2, depth, sub), F32),
            pltpu.VMEM((n, 2, 2, half), F32),
            pltpu.VMEM((n, 2, 2, half), F32),
            pltpu.VMEM((n, 2, 2, half), F32),
            pltpu.VMEM((n, 2, 1, half), F32),
            pltpu.VMEM((8, half), F32),
            pltpu.VMEM((n, 4, depth), F32),
            dma, dma, dma((2,)),
            dma((2, chips)), dma((2, chips)), dma((2, chips)), dma((2, chips)),
            dma((n,)), dma((n,)), dma((n,)), dma((n,)), dma((n,)), dma((n,)), dma((n,)), dma((n,)),
            dma((2, 2, 2)), dma((2, 2, 2)), dma((2, 2)), dma((2, 2)),
            pltpu.SemaphoreType.REGULAR((2,)), pltpu.SemaphoreType.REGULAR((2,)),
        ],
        compiler_params=pltpu.CompilerParams(
            collective_id=0, has_side_effects=True, vmem_limit_bytes=67000000),
        name="head",
    )(x, gain, bias, w, aux)


def solution(mesh):
    n = mesh.shape["vp"]

    def per_device(hidden, norm_gain, norm_bias, w_blk, labels, loss_mask):
        seq, batch, depth = hidden.shape
        tokens = seq * batch
        aux = jnp.stack(
            [labels.astype(F32).reshape(2, tokens // 2), loss_mask.reshape(2, tokens // 2)], axis=1)
        dx, dwt, dgain, dbias, loss, _ = head_call(
            n, hidden.reshape(tokens, depth), norm_gain.reshape(1, depth), norm_bias.reshape(1, depth), w_blk, aux)
        return loss[0, :1], dx.reshape(seq, batch, depth), dwt.T, dgain[0], dbias[0]

    tok_spec = P("vp", "dp")
    return jax.shard_map(
        per_device,
        mesh=mesh,
        in_specs=(P("vp", "dp", None), P(None), P(None), P(None, "vp"), tok_spec, tok_spec),
        out_specs=(P("dp"), P("vp", "dp", None), P("dp", "vp"), P("dp"), P("dp")),
        check_vma=False,
    )
```

```python
import functools

import jax
import jax.numpy as jnp
from jax import lax
from jax.experimental import pallas as pl
from jax.experimental.pallas import tpu as pltpu
from jax.sharding import PartitionSpec as P

NORM_EPS = 1e-5
F32 = jnp.float32
BF16 = jnp.bfloat16
MESH = pl.DeviceIdType.MESH


def row_chunk(rows, limit):
    best = 16
    for size in range(16, limit + 1, 16):
        if rows % size == 0:
            best = size
    return best


def head_kernel(
    n, x_hbm, affine_ref, w_hbm, aux_ref,
    dx_hbm, dwt_hbm, dgain_ref, dbias_ref, loss_ref, z_hbm,
    w_v, wt, h_all, dw_acc, z_even, z_odd, dzb, h_pair, own, give, ring_in, mate_in,
    aux_all, st_loc, st_all, lse_all, t_acc, fin_all,
    w_sem, dw_sem, x_sem, dx_sem, z_sem,
    f_send, f_recv, p_send, p_recv,
    a_send, a_recv, s_send, s_recv, l_send, l_recv, e_send, e_recv,
    r_send, r_recv, q_send, q_recv, r_cred, q_cred,
):
    chips = n // 2
    me = lax.axis_index("vp")
    zc, core = me // 2, me % 2
    mate = zc * 2 + 1 - core
    up = lax.rem(zc + 1, chips) * 2 + core
    down = lax.rem(zc + chips - 1, chips) * 2 + core
    ahead = (up, down)
    depth, cols = w_v.shape
    half = x_hbm.shape[1]
    tokens = 2 * half
    sub = half // 2
    vchunk = row_chunk(cols, 640)
    col_start = me * cols

    def remote(src, dst, send, recv, dev):
        return pltpu.make_async_remote_copy(
            src_ref=src, dst_ref=dst, send_sem=send, recv_sem=recv,
            device_id={"vp": dev}, device_id_type=MESH)

    def peer_of(k):
        return lax.rem(me + k, n)

    x_first = [pltpu.make_async_copy(x_hbm.at[hf], h_pair.at[pl.ds(hf * half, half)], x_sem.at[hf]) for hf in (0, 1)]
    for copy in x_first:
        copy.start()
    w_copy = pltpu.make_async_copy(w_hbm, w_v, w_sem)
    w_copy.start()

    barrier = pltpu.get_barrier_semaphore()
    for k in range(1, n):
        pl.semaphore_signal(barrier, inc=1, device_id={"vp": peer_of(k)}, device_id_type=MESH)

    gain = 1.0 + affine_ref[0:1, :]
    bias = affine_ref[1:2, :]

    def normed_rows(rows):
        xf = rows.astype(F32)
        centered = xf - jnp.mean(xf, axis=-1, keepdims=True)
        inv_std = lax.rsqrt(jnp.mean(centered * centered, axis=-1, keepdims=True) + NORM_EPS)
        return centered * inv_std, inv_std

    ln_rows = half // 4
    for copy in x_first:
        copy.wait()

    @pl.loop(0, 8)
    def _(i):
        row0 = pl.multiple_of((i % 4) * ln_rows, ln_rows)
        src0 = pl.multiple_of(i * ln_rows, ln_rows)
        normed, _ = normed_rows(h_pair[pl.ds(src0, ln_rows), :])
        h_all[me, i // 4, pl.ds(row0, ln_rows), :] = (normed * gain + bias).astype(BF16)

    aux_all[me] = aux_ref[...]
    t_acc[...] = jnp.zeros_like(t_acc)
    pl.semaphore_wait(barrier, n - 1)

    def ring_copy(d, k, blk, hf):
        ref = h_all.at[blk, hf]
        return remote(ref, ref, f_send.at[d, k], f_recv.at[d, k], ahead[d])

    def mate_copy(d, k, blk, hf):
        ref = h_all.at[blk, hf]
        return remote(ref, ref, p_send.at[d, k], p_recv.at[d, k], mate)

    def fwd_half(d, k):
        return (k + 1) % 2 if d == 0 else k % 2

    for k in (1, 2):
        for d in (0, 1):
            ring_copy(d, k, me, fwd_half(d, k)).start()

    def spread(ref, dst, send, recv):
        for k in range(1, n):
            remote(ref, dst, send.at[k], recv.at[me], peer_of(k)).start()

    def collect(ref_all, send, recv):
        for k in range(1, n):
            src = peer_of(k)
            remote(ref_all.at[src], ref_all.at[src], send.at[k], recv.at[src], src).wait_recv()

    def drain(ref, send, recv):
        for k in range(1, n):
            remote(ref, ref, send.at[k], recv.at[me], peer_of(k)).wait_send()

    spread(aux_all.at[me], aux_all.at[me], a_send, a_recv)

    w_copy.wait()
    tcols = 128 if cols % 128 == 0 else cols

    @pl.loop(0, cols // tcols)
    def _(i):
        c0 = pl.multiple_of(i * tcols, tcols)
        wt[pl.ds(c0, tcols), :] = w_v[:, pl.ds(c0, tcols)].T

    last = chips - 1

    z_stage = (z_even, z_odd)
    dz_refs = (dzb, wt.at[:, pl.ds(0, tokens)])

    def z_out(side, d, tile):
        src = z_stage[side].at[:, pl.ds(d * half, half)]
        return pltpu.make_async_copy(src, z_hbm.at[tile], z_sem.at[side, d])

    def fwd_chip(d, k):
        step = (k + 1) // 2
        return lax.rem(zc + chips - step, chips) if d == 0 else lax.rem(zc + step, chips)

    @pl.loop(0, chips)
    def _(k):
        for d in (0, 1):
            blk = fwd_chip(d, k) * 2 + core
            hf = fwd_half(d, k)

            @pl.when(k >= 1)
            def _():
                ring_copy(d, k, blk, hf).wait_recv()

                @pl.when(k + 2 <= last)
                def _():
                    ring_copy(d, k + 2, blk, hf).start()

            mate_copy(d, k, blk, hf).start()

        for side in (0, 1):
            places = [(fwd_chip(d, k) * 2 + (core if side == 0 else 1 - core), fwd_half(d, k)) for d in (0, 1)]
            for d in (0, 1):
                if side == 1:
                    mate_copy(d, k, *places[d]).wait_recv()
                h_pair[pl.ds(d * half, half), :] = h_all[places[d]]

            @pl.when(k >= 1)
            def _():
                for d in (0, 1):
                    z_out(side, d, 0).wait()

            m8 = jnp.full((8, tokens), -jnp.inf, F32)
            s8 = jnp.zeros((8, tokens), F32)
            h_tile = h_pair[...]
            for j in range(cols // vchunk):
                rows = pl.ds(j * vchunk, vchunk)
                z = lax.dot_general(wt[rows, :], h_tile, (((1,), (1,)), ((), ())), preferred_element_type=F32)
                z_stage[side][rows, 0:tokens] = z
                z3 = z.reshape(vchunk // 8, 8, tokens)
                m_new = jnp.maximum(m8, jnp.max(z3, axis=0))
                s8 = s8 * jnp.exp(m8 - m_new) + jnp.sum(jnp.exp(z3 - m_new[None]), axis=0)
                m8 = m_new
            m1 = jnp.max(m8, axis=0, keepdims=True)
            s1 = jnp.sum(s8 * jnp.exp(m8 - m1), axis=0, keepdims=True)
            for d in (0, 1):
                blk, hf = places[d]
                lanes = slice(d * half, (d + 1) * half)
                st_loc[blk, hf, 0:1, :] = m1[:, lanes]
                st_loc[blk, hf, 1:2, :] = s1[:, lanes]
                z_out(side, d, blk * 2 + hf).start()

    def bwd_chip(d, s):
        return lax.rem(zc + 2 * chips + (2 * d - 1) * (s + 1), chips)

    def z_in(side, d, s):
        blk = bwd_chip(d, s) * 2 + (core if side == 0 else 1 - core)
        return pltpu.make_async_copy(z_hbm.at[blk * 2 + d], z_stage[d].at[:, pl.ds(side * half, half)], z_sem.at[d, side])

    for k in range(1, n):
        peer = peer_of(k)
        remote(st_loc.at[peer], st_all.at[me], s_send.at[k], s_recv.at[me], peer).start()
    st_all[me] = st_loc[me]
    for side in (0, 1):
        for d in (0, 1):
            z_out(side, d, 0).wait()
    for d in (0, 1):
        for side in (0, 1):
            z_in(side, d, 0).start()

    @pl.loop(0, cols // vchunk)
    def _(i):
        c0 = pl.multiple_of(i * vchunk, vchunk)
        dw_acc[pl.ds(c0, vchunk), :] = jnp.zeros((vchunk, depth), F32)

    collect(st_all, s_send, s_recv)
    for hf in (0, 1):
        tops = [st_all[i, hf, 0:1, :] for i in range(n)]
        top = functools.reduce(jnp.maximum, tops)
        total = functools.reduce(jnp.add, [st_all[i, hf, 1:2, :] * jnp.exp(tops[i] - top) for i in range(n)])
        lse_all[me, hf] = top + jnp.log(total)
    spread(lse_all.at[me], lse_all.at[me], l_send, l_recv)
    collect(aux_all, a_send, a_recv)
    mask_sum = functools.reduce(jnp.add, [aux_all[i, hf, 1:2, :] for i in range(n) for hf in (0, 1)])
    mask_total = jnp.sum(mask_sum, axis=1, keepdims=True)
    collect(lse_all, l_send, l_recv)
    for k in range(1, chips):
        for d in (0, 1):
            ring_copy(d, k, me, 0).wait_send()
    for k in range(chips):
        for d in (0, 1):
            mate_copy(d, k, me, 0).wait_send()

    def ring_sum(d, slot, sb):
        return remote(own.at[d, slot, sb], ring_in.at[d, slot, sb], r_send.at[d, slot, sb], r_recv.at[d, slot, sb],
                      ahead[d])

    def mate_sum(d, slot):
        return remote(give.at[d], mate_in.at[d, slot], q_send.at[d], q_recv.at[d, slot], mate)

    def event(d, s, sb):
        slot = lax.rem(s, 2)
        prev = lax.rem(s + 1, 2)
        if sb == 0:
            mate_sum(d, slot).wait_recv()

        @pl.when(s == 0)
        def _():
            own[d, slot, sb] = own[d, slot, sb] + mate_in[d, slot, sb]

        @pl.when(s >= 1)
        def _():
            ring_sum(d, prev, sb).wait_recv()
            own[d, slot, sb] = (own[d, slot, sb] + mate_in[d, slot, sb]) + ring_in[d, prev, sb]

        @pl.when(s <= chips - 2)
        def _():
            if sb == 0:
                @pl.when(s >= 2)
                def _():
                    pl.semaphore_wait(r_cred.at[d], 1)
            ring_sum(d, slot, sb).start()

        if sb == 1:
            @pl.when((s >= 1) & (s <= chips - 3))
            def _():
                pl.semaphore_signal(r_cred.at[d], inc=1, device_id={"vp": ahead[1 - d]}, device_id_type=MESH)

            @pl.when(s <= chips - 3)
            def _():
                pl.semaphore_signal(q_cred.at[d], inc=1, device_id={"vp": mate}, device_id_type=MESH)

    kchunk = 768 if cols > 768 else cols

    def dz_rows(d, blk, lanes, r0, size):
        lab = aux_all[blk, d, 0:1, :].astype(jnp.int32) - (col_start + r0)
        weight = aux_all[blk, d, 1:2, :] / mask_total
        z = z_stage[d][pl.ds(r0, size), lanes]
        hit = lax.broadcasted_iota(jnp.int32, (size, half), 0) == lab
        prob = jnp.exp(z - lse_all[blk, d])
        dz_refs[d][pl.ds(r0, size), lanes] = (jnp.where(hit, prob - 1.0, prob) * weight).astype(BF16)
        return jnp.sum(jnp.where(hit, z, 0.0).reshape(size // 8, 8, half), axis=0)

    @pl.loop(0, chips)
    def _(s):
        slot = lax.rem(s, 2)
        for d in (0, 1):
            for side in (0, 1):
                z_in(side, d, s).wait()

            @pl.when(s >= 1)
            def _():
                mate_sum(d, slot).wait_send()

            @pl.when(s >= 2)
            def _():
                for sb in (0, 1):
                    ring_sum(d, slot, sb).wait_send()

            blks = [bwd_chip(d, s) * 2 + (core if side == 0 else 1 - core) for side in (0, 1)]
            t8 = [jnp.zeros((8, half), F32), jnp.zeros((8, half), F32)]
            g = jnp.zeros((depth, tokens), F32)
            for r0 in range(0, cols, kchunk):
                size = min(kchunk, cols - r0)
                for side in (0, 1):
                    t8[side] = t8[side] + dz_rows(d, blks[side], slice(side * half, (side + 1) * half), r0, size)
                g = g + jnp.dot(w_v[:, r0:r0 + size], dz_refs[d][r0:r0 + size, :], preferred_element_type=F32)
            for side in (0, 1):
                t_acc[...] += t8[side] * aux_all[blks[side], d, 1:2, :]
            for sb in (0, 1):
                own[d, slot, sb] = g[:, sb * sub:(sb + 1) * sub]
                give[d, sb] = g[:, half + sb * sub:half + (sb + 1) * sub]

            @pl.when(s + 1 < chips)
            def _():
                for side in (0, 1):
                    z_in(side, d, s + 1).start()

            @pl.when(s >= 2)
            def _():
                pl.semaphore_wait(q_cred.at[d], 1)
            mate_sum(d, slot).start()

        for d in (0, 1):
            event(d, s, 0)

        for d in (0, 1):
            chip = bwd_chip(d, s)
            h_pair[0:half, :] = h_all[chip * 2 + core, d]
            h_pair[half:tokens, :] = h_all[chip * 2 + 1 - core, d]
            h_tile = h_pair[...]
            for i in range(cols // vchunk):
                rows = pl.ds(i * vchunk, vchunk)
                dw_acc[rows, :] += jnp.dot(dz_refs[d][rows, :], h_tile, preferred_element_type=F32)

        @pl.when(s < chips - 1)
        def _():
            for d in (0, 1):
                event(d, s, 1)

    dw_copy = pltpu.make_async_copy(dw_acc, dwt_hbm, dw_sem)
    dw_copy.start()
    x_again = pltpu.make_async_copy(x_hbm, h_all.at[0], x_sem.at[0])
    x_again.start()
    for d in (0, 1):
        event(d, chips - 1, 1)

    x_again.wait()
    last_slot = (chips - 1) % 2
    dg = jnp.zeros((1, depth), F32)
    dc = jnp.zeros((1, depth), F32)
    for hf in (0, 1):
        for sb in (0, 1):
            rows = slice(sb * sub, (sb + 1) * sub)
            dh = own[hf, last_slot, sb].T
            normed, inv_std = normed_rows(h_all[0, hf, rows, :])
            dg = dg + jnp.sum(dh * normed, axis=0, keepdims=True)
            dc = dc + jnp.sum(dh, axis=0, keepdims=True)
            scaled = dh * gain
            mean_q = jnp.mean(scaled, axis=-1, keepdims=True)
            mean_qn = jnp.mean(scaled * normed, axis=-1, keepdims=True)
            h_all[1, hf, rows, :] = (inv_std * (scaled - mean_q - normed * mean_qn)).astype(BF16)
    dx_copy = pltpu.make_async_copy(h_all.at[1], dx_hbm, dx_sem)
    dx_copy.start()
    fin_all[me, 0:1, :] = dg
    fin_all[me, 1:2, :] = dc
    t_here = jnp.sum(jnp.sum(t_acc[...], axis=0, keepdims=True), axis=1, keepdims=True)
    fin_all[me, 2:3, :] = jnp.broadcast_to(t_here, (1, depth))
    fin_all[me, 3:4, :] = jnp.zeros((1, depth), F32)
    spread(fin_all.at[me], fin_all.at[me], e_send, e_recv)
    lse_sum = functools.reduce(
        jnp.add, [aux_all[i, hf, 1:2, :] * lse_all[i, hf] for i in range(n) for hf in (0, 1)])
    lse_total = jnp.sum(lse_sum, axis=1, keepdims=True)
    collect(fin_all, e_send, e_recv)
    dgain_ref[...] = functools.reduce(jnp.add, [fin_all[i, 0:1, :] for i in range(n)])
    dbias_ref[...] = functools.reduce(jnp.add, [fin_all[i, 1:2, :] for i in range(n)])
    t_total = functools.reduce(jnp.add, [fin_all[i, 2:3, 0:128] for i in range(n)])
    loss_ref[...] = (lse_total - t_total) / mask_total

    drain(aux_all.at[me], a_send, a_recv)
    drain(st_loc.at[me], s_send, s_recv)
    drain(lse_all.at[me], l_send, l_recv)
    drain(fin_all.at[me], e_send, e_recv)
    for d in (0, 1):
        for sb in (0, 1):
            ring_sum(d, (chips - 2) % 2, sb).wait_send()
        mate_sum(d, 0).wait_send()
    dw_copy.wait()
    dx_copy.wait()


def head_call(n, x, affine, w, aux):
    _, half, depth = x.shape
    tokens = 2 * half
    cols = w.shape[1]
    sub = half // 2
    chips = n // 2
    vmem = pl.BlockSpec(memory_space=pltpu.VMEM)
    anywhere = pl.BlockSpec(memory_space=pl.ANY)
    dma = pltpu.SemaphoreType.DMA
    return pl.pallas_call(
        functools.partial(head_kernel, n),
        out_shape=(
            jax.ShapeDtypeStruct((2, half, depth), BF16),
            jax.ShapeDtypeStruct((cols, depth), F32),
            jax.ShapeDtypeStruct((1, depth), F32),
            jax.ShapeDtypeStruct((1, depth), F32),
            jax.ShapeDtypeStruct((1, 128), F32),
            jax.ShapeDtypeStruct((2 * n, cols, half), F32),
        ),
        in_specs=[anywhere, vmem, anywhere, vmem],
        out_specs=(anywhere, anywhere, vmem, vmem, vmem, anywhere),
        scratch_shapes=[
            pltpu.VMEM((depth, cols), BF16),
            pltpu.VMEM((cols, depth), BF16),
            pltpu.VMEM((n, 2, half, depth), BF16),
            pltpu.VMEM((cols, depth), F32),
            pltpu.VMEM((cols, tokens), F32),
            pltpu.VMEM((cols, tokens), F32),
            pltpu.VMEM((cols, tokens), BF16),
            pltpu.VMEM((tokens, depth), BF16),
            pltpu.VMEM((2, 2, 2, depth, sub), F32),
            pltpu.VMEM((2, 2, depth, sub), F32),
            pltpu.VMEM((2, 2, 2, depth, sub), F32),
            pltpu.VMEM((2, 2, 2, depth, sub), F32),
            pltpu.VMEM((n, 2, 2, half), F32),
            pltpu.VMEM((n, 2, 2, half), F32),
            pltpu.VMEM((n, 2, 2, half), F32),
            pltpu.VMEM((n, 2, 1, half), F32),
            pltpu.VMEM((8, half), F32),
            pltpu.VMEM((n, 4, depth), F32),
            dma, dma, dma((2,)), dma, dma((2, 2)),
            dma((2, chips)), dma((2, chips)), dma((2, chips)), dma((2, chips)),
            dma((n,)), dma((n,)), dma((n,)), dma((n,)), dma((n,)), dma((n,)), dma((n,)), dma((n,)),
            dma((2, 2, 2)), dma((2, 2, 2)), dma((2,)), dma((2, 2)),
            pltpu.SemaphoreType.REGULAR((2,)), pltpu.SemaphoreType.REGULAR((2,)),
        ],
        compiler_params=pltpu.CompilerParams(
            collective_id=0, has_side_effects=True, vmem_limit_bytes=67000000),
        name="head",
    )(x, affine, w, aux)


def flip_kernel(x_ref, y_ref):
    y_ref[...] = x_ref[...].T


def flip(x):
    rows, depth = x.shape
    size = 640 if rows % 640 == 0 else rows
    return pl.pallas_call(
        flip_kernel,
        grid=(rows // size,),
        out_shape=jax.ShapeDtypeStruct((depth, rows), x.dtype),
        in_specs=[pl.BlockSpec((size, depth), lambda i: (i, 0))],
        out_specs=pl.BlockSpec((depth, size), lambda i: (0, i)),
        name="flip",
    )(x)


def solution(mesh):
    n = mesh.shape["vp"]

    def per_device(hidden, norm_gain, norm_bias, w_blk, labels, loss_mask):
        seq, batch, depth = hidden.shape
        tokens = seq * batch
        aux = jnp.stack(
            [labels.astype(F32).reshape(2, tokens // 2), loss_mask.reshape(2, tokens // 2)], axis=1)
        dx, dwt, dgain, dbias, loss, _ = head_call(
            n, hidden.reshape(2, tokens // 2, depth), jnp.stack([norm_gain, norm_bias]), w_blk, aux)
        return loss[0, :1], dx.reshape(seq, batch, depth), flip(dwt), dgain[0], dbias[0]

    tok_spec = P("vp", "dp")
    return jax.shard_map(
        per_device,
        mesh=mesh,
        in_specs=(P("vp", "dp", None), P(None), P(None), P(None, "vp"), tok_spec, tok_spec),
        out_specs=(P("dp"), P("vp", "dp", None), P("dp", "vp"), P("dp"), P("dp")),
        check_vma=False,
    )
```

```python
import functools

import jax
import jax.numpy as jnp
from jax import lax
from jax.experimental import pallas as pl
from jax.experimental.pallas import tpu as pltpu
from jax.sharding import PartitionSpec as P

NORM_EPS = 1e-5
F32 = jnp.float32
BF16 = jnp.bfloat16
MESH = pl.DeviceIdType.MESH


def row_chunk(rows, limit):
    best = 16
    for size in range(16, limit + 1, 16):
        if rows % size == 0:
            best = size
    return best


def head_kernel(
    n, x_hbm, gain_ref, bias_ref, w_hbm, aux_ref,
    dx_hbm, dw_hbm, dgain_ref, dbias_ref, loss_ref, z_hbm,
    w_v, wt, h_all, dw_acc, z_even, z_odd, dzb, h_pair, own, give, ring_in, mate_in,
    aux_all, st_loc, st_all, part_all, far_all, lse_all, t_acc, fin_all,
    w_sem, dw_sem, x_sem, dx_sem, z_sem,
    f_send, f_recv, p_send, p_recv,
    a_send, a_recv, s_send, s_recv, c_send, c_recv, l_send, l_recv, e_send, e_recv,
    r_send, r_recv, q_send, q_recv, r_cred, q_cred,
):
    chips = n // 2
    me = lax.axis_index("vp")
    zc, core = me // 2, me % 2
    mate = zc * 2 + 1 - core
    up = lax.rem(zc + 1, chips) * 2 + core
    down = lax.rem(zc + chips - 1, chips) * 2 + core
    ahead = (up, down)
    depth, cols = w_v.shape
    half = x_hbm.shape[1]
    tokens = 2 * half
    sub = half // 2
    vchunk = row_chunk(cols, 640)
    col_start = me * cols

    def remote(src, dst, send, recv, dev):
        return pltpu.make_async_remote_copy(
            src_ref=src, dst_ref=dst, send_sem=send, recv_sem=recv,
            device_id={"vp": dev}, device_id_type=MESH)

    def peer_of(k):
        return lax.rem(me + k, n)

    x_first = [pltpu.make_async_copy(x_hbm.at[hf], h_pair.at[pl.ds(hf * half, half)], x_sem.at[hf]) for hf in (0, 1)]
    for copy in x_first:
        copy.start()
    w_copy = pltpu.make_async_copy(w_hbm, w_v, w_sem)
    w_copy.start()

    barrier = pltpu.get_barrier_semaphore()
    for k in range(1, n):
        pl.semaphore_signal(barrier, inc=1, device_id={"vp": peer_of(k)}, device_id_type=MESH)

    gain = 1.0 + gain_ref[...].reshape(1, depth)
    bias = bias_ref[...].reshape(1, depth)

    def normed_rows(rows):
        xf = rows.astype(F32)
        centered = xf - jnp.mean(xf, axis=-1, keepdims=True)
        inv_std = lax.rsqrt(jnp.mean(centered * centered, axis=-1, keepdims=True) + NORM_EPS)
        return centered * inv_std, inv_std

    ln_rows = half // 4
    for copy in x_first:
        copy.wait()

    @pl.loop(0, 8)
    def _(i):
        row0 = pl.multiple_of((i % 4) * ln_rows, ln_rows)
        src0 = pl.multiple_of(i * ln_rows, ln_rows)
        normed, _ = normed_rows(h_pair[pl.ds(src0, ln_rows), :])
        h_all[me, i // 4, pl.ds(row0, ln_rows), :] = (normed * gain + bias).astype(BF16)

    aux_all[me] = aux_ref[...]
    t_acc[...] = jnp.zeros_like(t_acc)
    pl.semaphore_wait(barrier, n - 1)

    def ring_copy(d, k, blk, hf):
        ref = h_all.at[blk, hf]
        return remote(ref, ref, f_send.at[d, k], f_recv.at[d, k], ahead[d])

    def mate_copy(d, k, blk, hf):
        ref = h_all.at[blk, hf]
        return remote(ref, ref, p_send.at[d, k], p_recv.at[d, k], mate)

    def fwd_half(d, k):
        return (k + 1) % 2 if d == 0 else k % 2

    for k in (1, 2):
        for d in (0, 1):
            ring_copy(d, k, me, fwd_half(d, k)).start()

    def spread(ref, dst, send, recv):
        for k in range(1, n):
            remote(ref, dst, send.at[k], recv.at[me], peer_of(k)).start()

    def collect(ref_all, send, recv):
        for k in range(1, n):
            src = peer_of(k)
            remote(ref_all.at[src], ref_all.at[src], send.at[k], recv.at[src], src).wait_recv()

    def drain(ref, send, recv):
        for k in range(1, n):
            remote(ref, ref, send.at[k], recv.at[me], peer_of(k)).wait_send()

    spread(aux_all.at[me], aux_all.at[me], a_send, a_recv)

    w_copy.wait()
    tcols = 128 if cols % 128 == 0 else cols

    @pl.loop(0, cols // tcols)
    def _(i):
        c0 = pl.multiple_of(i * tcols, tcols)
        wt[pl.ds(c0, tcols), :] = w_v[:, pl.ds(c0, tcols)].T

    last = chips - 1
    far = lax.rem(zc + chips // 2, chips)
    near = [(dc * 2 + cc, lax.rem(zc + dc, chips) * 2 + (core if cc == 0 else 1 - core))
            for dc in range(chips) for cc in (0, 1) if dc != chips // 2 and (dc, cc) != (0, 0)]

    def near_copy(i, dev):
        return remote(st_loc.at[dev], st_all.at[me], s_send.at[i], s_recv.at[me], dev)

    def join(pairs):
        top = functools.reduce(jnp.maximum, [m for m, _ in pairs])
        return top, functools.reduce(jnp.add, [t * jnp.exp(m - top) for m, t in pairs])

    def stat(ref, *at):
        return ref[(*at, slice(0, 1))], ref[(*at, slice(1, 2))]

    def join_near():
        for _, dev in near:
            remote(st_all.at[dev], st_all.at[dev], s_send.at[0], s_recv.at[dev], dev).wait_recv()
        for hf in (0, 1):
            top, total = join([stat(st_loc, me, hf)] + [stat(st_all, dev, hf) for _, dev in near])
            part_all[me, hf, 0:1, :] = top
            part_all[me, hf, 1:2, :] = total
        spread(part_all.at[me], part_all.at[me], l_send, l_recv)

    z_stage = (z_even, z_odd)
    dz_refs = (dzb, wt.at[:, pl.ds(0, tokens)])

    def z_out(side, d, tile):
        src = z_stage[side].at[:, pl.ds(d * half, half)]
        return pltpu.make_async_copy(src, z_hbm.at[tile], z_sem.at[side, d])

    def fwd_chip(d, k):
        step = (k + 1) // 2
        return lax.rem(zc + chips - step, chips) if d == 0 else lax.rem(zc + step, chips)

    @pl.loop(0, chips)
    def _(k):
        for d in (0, 1):
            blk = fwd_chip(d, k) * 2 + core
            hf = fwd_half(d, k)

            @pl.when(k >= 1)
            def _():
                ring_copy(d, k, blk, hf).wait_recv()

                @pl.when(k + 2 <= last)
                def _():
                    ring_copy(d, k + 2, blk, hf).start()

            mate_copy(d, k, blk, hf).start()

        for side in (0, 1):
            places = [(fwd_chip(d, k) * 2 + (core if side == 0 else 1 - core), fwd_half(d, k)) for d in (0, 1)]
            for d in (0, 1):
                if side == 1:
                    mate_copy(d, k, *places[d]).wait_recv()
                h_pair[pl.ds(d * half, half), :] = h_all[places[d]]

            @pl.when(k >= 1)
            def _():
                for d in (0, 1):
                    z_out(side, d, 0).wait()

            m8 = jnp.full((8, tokens), -jnp.inf, F32)
            s8 = jnp.zeros((8, tokens), F32)
            h_tile = h_pair[...]
            for j in range(cols // vchunk):
                rows = pl.ds(j * vchunk, vchunk)
                z = lax.dot_general(wt[rows, :], h_tile, (((1,), (1,)), ((), ())), preferred_element_type=F32)
                z_stage[side][rows, 0:tokens] = z
                z3 = z.reshape(vchunk // 8, 8, tokens)
                m_new = jnp.maximum(m8, jnp.max(z3, axis=0))
                s8 = s8 * jnp.exp(m8 - m_new) + jnp.sum(jnp.exp(z3 - m_new[None]), axis=0)
                m8 = m_new
            m1 = jnp.max(m8, axis=0, keepdims=True)
            s1 = jnp.sum(s8 * jnp.exp(m8 - m1), axis=0, keepdims=True)
            for d in (0, 1):
                blk, hf = places[d]
                lanes = slice(d * half, (d + 1) * half)
                st_loc[blk, hf, 0:1, :] = m1[:, lanes]
                st_loc[blk, hf, 1:2, :] = s1[:, lanes]
                z_out(side, d, blk * 2 + hf).start()

            if side == 0:
                pl.when(k == last)(join_near)

        @pl.when(k == last - 1)
        def _():
            for i, dev in near:
                near_copy(i, dev).start()

    def bwd_chip(d, s):
        return lax.rem(zc + 2 * chips + (2 * d - 1) * (s + 1), chips)

    def z_in(side, d, s):
        blk = bwd_chip(d, s) * 2 + (core if side == 0 else 1 - core)
        return pltpu.make_async_copy(z_hbm.at[blk * 2 + d], z_stage[d].at[:, pl.ds(side * half, half)], z_sem.at[d, side])

    far_part = st_loc.at[pl.ds(far * 2, 2)]
    spread(far_part, far_all.at[me], c_send, c_recv)
    far_all[me] = far_part[...]
    for side in (0, 1):
        for d in (0, 1):
            z_out(side, d, 0).wait()
    for d in (0, 1):
        for side in (0, 1):
            z_in(side, d, 0).start()

    zrows = row_chunk(depth, 96)

    @pl.loop(0, depth // zrows)
    def _(i):
        r0 = pl.multiple_of(i * zrows, zrows)
        dw_acc[pl.ds(r0, zrows), :] = jnp.zeros((zrows, cols), F32)

    collect(aux_all, a_send, a_recv)
    mask_sum = functools.reduce(jnp.add, [aux_all[i, hf, 1:2, :] for i in range(n) for hf in (0, 1)])
    mask_total = jnp.sum(mask_sum, axis=1, keepdims=True)
    collect(part_all, l_send, l_recv)
    collect(far_all, c_send, c_recv)

    @pl.loop(0, n)
    def _(b):
        other = lax.rem(b // 2 + chips // 2, chips) * 2
        for hf in (0, 1):
            top, total = join([stat(part_all, b, hf)] + [stat(far_all, other + cc, lax.rem(b, 2), hf) for cc in (0, 1)])
            lse_all[b, hf] = top + jnp.log(total)

    for k in range(1, chips):
        for d in (0, 1):
            ring_copy(d, k, me, 0).wait_send()
    for k in range(chips):
        for d in (0, 1):
            mate_copy(d, k, me, 0).wait_send()

    def ring_sum(d, slot, sb):
        return remote(own.at[d, slot, sb], ring_in.at[d, slot, sb], r_send.at[d, slot, sb], r_recv.at[d, slot, sb],
                      ahead[d])

    def mate_sum(d, slot):
        return remote(give.at[d], mate_in.at[d, slot], q_send.at[d], q_recv.at[d, slot], mate)

    def event(d, s, sb):
        slot = lax.rem(s, 2)
        prev = lax.rem(s + 1, 2)
        if sb == 0:
            mate_sum(d, slot).wait_recv()

        @pl.when(s == 0)
        def _():
            own[d, slot, sb] = own[d, slot, sb] + mate_in[d, slot, sb]

        @pl.when(s >= 1)
        def _():
            ring_sum(d, prev, sb).wait_recv()
            own[d, slot, sb] = (own[d, slot, sb] + mate_in[d, slot, sb]) + ring_in[d, prev, sb]

        @pl.when(s <= chips - 2)
        def _():
            if sb == 0:
                @pl.when(s >= 2)
                def _():
                    pl.semaphore_wait(r_cred.at[d], 1)
            ring_sum(d, slot, sb).start()

        if sb == 1:
            @pl.when((s >= 1) & (s <= chips - 3))
            def _():
                pl.semaphore_signal(r_cred.at[d], inc=1, device_id={"vp": ahead[1 - d]}, device_id_type=MESH)

            @pl.when(s <= chips - 3)
            def _():
                pl.semaphore_signal(q_cred.at[d], inc=1, device_id={"vp": mate}, device_id_type=MESH)

    kchunk = 768 if cols > 768 else cols
    nchunk = 512 if cols > 512 else cols
    ht_refs = [wt.at[pl.ds(side * depth, depth), pl.ds(tokens, half)] for side in (0, 1)]

    def dz_rows(d, blk, lanes, r0, size):
        lab = aux_all[blk, d, 0:1, :].astype(jnp.int32) - (col_start + r0)
        weight = aux_all[blk, d, 1:2, :] / mask_total
        z = z_stage[d][pl.ds(r0, size), lanes]
        hit = lax.broadcasted_iota(jnp.int32, (size, half), 0) == lab
        prob = jnp.exp(z - lse_all[blk, d])
        dz_refs[d][pl.ds(r0, size), lanes] = (jnp.where(hit, prob - 1.0, prob) * weight).astype(BF16)
        return jnp.sum(jnp.where(hit, z, 0.0).reshape(size // 8, 8, half), axis=0)

    @pl.loop(0, chips)
    def _(s):
        slot = lax.rem(s, 2)
        for d in (0, 1):
            for side in (0, 1):
                z_in(side, d, s).wait()

            @pl.when(s >= 1)
            def _():
                mate_sum(d, slot).wait_send()

            @pl.when(s >= 2)
            def _():
                for sb in (0, 1):
                    ring_sum(d, slot, sb).wait_send()

            blks = [bwd_chip(d, s) * 2 + (core if side == 0 else 1 - core) for side in (0, 1)]
            t8 = [jnp.zeros((8, half), F32), jnp.zeros((8, half), F32)]
            g = jnp.zeros((depth, tokens), F32)
            for r0 in range(0, cols, kchunk):
                size = min(kchunk, cols - r0)
                for side in (0, 1):
                    t8[side] = t8[side] + dz_rows(d, blks[side], slice(side * half, (side + 1) * half), r0, size)
                g = g + jnp.dot(w_v[:, r0:r0 + size], dz_refs[d][r0:r0 + size, :], preferred_element_type=F32)
            for side in (0, 1):
                t_acc[...] += t8[side] * aux_all[blks[side], d, 1:2, :]
            for sb in (0, 1):
                own[d, slot, sb] = g[:, sb * sub:(sb + 1) * sub]
                give[d, sb] = g[:, half + sb * sub:half + (sb + 1) * sub]

            @pl.when(s + 1 < chips)
            def _():
                for side in (0, 1):
                    z_in(side, d, s + 1).start()

            @pl.when(s >= 2)
            def _():
                pl.semaphore_wait(q_cred.at[d], 1)
            mate_sum(d, slot).start()

        for d in (0, 1):
            event(d, s, 0)

        for d in (0, 1):
            for side in (0, 1):
                blk = bwd_chip(d, s) * 2 + (core if side == 0 else 1 - core)
                ht_refs[side][...] = h_all[blk, d].T
            for r0 in range(0, cols, nchunk):
                size = min(nchunk, cols - r0)
                parts = [
                    lax.dot_general(ht_refs[side][...], dz_refs[d][r0:r0 + size, side * half:(side + 1) * half],
                                    (((1,), (1,)), ((), ())), preferred_element_type=F32) for side in (0, 1)]
                dw_acc[:, r0:r0 + size] += parts[0] + parts[1]

        @pl.when(s < chips - 1)
        def _():
            for d in (0, 1):
                event(d, s, 1)

    dw_copy = pltpu.make_async_copy(dw_acc, dw_hbm, dw_sem)
    dw_copy.start()
    x_again = pltpu.make_async_copy(x_hbm, h_all.at[0], x_sem.at[0])
    x_again.start()
    last_slot = (chips - 1) % 2
    x_again.wait()
    dg = jnp.zeros((1, depth), F32)
    dc = jnp.zeros((1, depth), F32)
    for sb in (0, 1):
        if sb == 1:
            for d in (0, 1):
                event(d, chips - 1, 1)
        for hf in (0, 1):
            rows = slice(sb * sub, (sb + 1) * sub)
            dh = own[hf, last_slot, sb].T
            normed, inv_std = normed_rows(h_all[0, hf, rows, :])
            dg = dg + jnp.sum(dh * normed, axis=0, keepdims=True)
            dc = dc + jnp.sum(dh, axis=0, keepdims=True)
            scaled = dh * gain
            mean_q = jnp.mean(scaled, axis=-1, keepdims=True)
            mean_qn = jnp.mean(scaled * normed, axis=-1, keepdims=True)
            h_all[1, hf, rows, :] = (inv_std * (scaled - mean_q - normed * mean_qn)).astype(BF16)
    dx_copy = pltpu.make_async_copy(h_all.at[1], dx_hbm, dx_sem)
    dx_copy.start()
    fin_all[me, 0:1, :] = dg
    fin_all[me, 1:2, :] = dc
    t_here = jnp.sum(jnp.sum(t_acc[...], axis=0, keepdims=True), axis=1, keepdims=True)
    fin_all[me, 2:3, :] = jnp.broadcast_to(t_here, (1, depth))
    fin_all[me, 3:4, :] = jnp.zeros((1, depth), F32)
    spread(fin_all.at[me], fin_all.at[me], e_send, e_recv)
    lse_sum = functools.reduce(
        jnp.add, [aux_all[i, hf, 1:2, :] * lse_all[i, hf] for i in range(n) for hf in (0, 1)])
    lse_total = jnp.sum(lse_sum, axis=1, keepdims=True)
    collect(fin_all, e_send, e_recv)
    dgain_ref[...] = functools.reduce(jnp.add, [fin_all[i, 0:1, :] for i in range(n)]).reshape(depth)
    dbias_ref[...] = functools.reduce(jnp.add, [fin_all[i, 1:2, :] for i in range(n)]).reshape(depth)
    t_total = functools.reduce(jnp.add, [fin_all[i, 2:3, 0:128] for i in range(n)])
    loss_ref[...] = (lse_total - t_total) / mask_total

    drain(aux_all.at[me], a_send, a_recv)
    for i, dev in near:
        near_copy(i, dev).wait_send()
    drain(part_all.at[me], l_send, l_recv)
    drain(far_all.at[me], c_send, c_recv)
    drain(fin_all.at[me], e_send, e_recv)
    for d in (0, 1):
        for sb in (0, 1):
            ring_sum(d, (chips - 2) % 2, sb).wait_send()
        mate_sum(d, 0).wait_send()
    dw_copy.wait()
    dx_copy.wait()


def head_call(n, x, gain, bias, w, aux):
    _, half, depth = x.shape
    tokens = 2 * half
    cols = w.shape[1]
    sub = half // 2
    chips = n // 2
    vmem = pl.BlockSpec(memory_space=pltpu.VMEM)
    anywhere = pl.BlockSpec(memory_space=pl.ANY)
    dma = pltpu.SemaphoreType.DMA
    return pl.pallas_call(
        functools.partial(head_kernel, n),
        out_shape=(
            jax.ShapeDtypeStruct((2, half, depth), BF16),
            jax.ShapeDtypeStruct((depth, cols), F32),
            jax.ShapeDtypeStruct((depth,), F32),
            jax.ShapeDtypeStruct((depth,), F32),
            jax.ShapeDtypeStruct((1, 128), F32),
            jax.ShapeDtypeStruct((2 * n, cols, half), F32),
        ),
        in_specs=[anywhere, vmem, vmem, anywhere, vmem],
        out_specs=(anywhere, anywhere, vmem, vmem, vmem, anywhere),
        scratch_shapes=[
            pltpu.VMEM((depth, cols), BF16),
            pltpu.VMEM((cols, depth), BF16),
            pltpu.VMEM((n, 2, half, depth), BF16),
            pltpu.VMEM((depth, cols), F32),
            pltpu.VMEM((cols, tokens), F32),
            pltpu.VMEM((cols, tokens), F32),
            pltpu.VMEM((cols, tokens), BF16),
            pltpu.VMEM((tokens, depth), BF16),
            pltpu.VMEM((2, 2, 2, depth, sub), F32),
            pltpu.VMEM((2, 2, depth, sub), F32),
            pltpu.VMEM((2, 2, 2, depth, sub), F32),
            pltpu.VMEM((2, 2, 2, depth, sub), F32),
            pltpu.VMEM((n, 2, 2, half), F32),
            pltpu.VMEM((n, 2, 2, half), F32),
            pltpu.VMEM((n, 2, 2, half), F32),
            pltpu.VMEM((n, 2, 2, half), F32),
            pltpu.VMEM((n, 2, 2, 2, half), F32),
            pltpu.VMEM((n, 2, 1, half), F32),
            pltpu.VMEM((8, half), F32),
            pltpu.VMEM((n, 4, depth), F32),
            dma, dma, dma((2,)), dma, dma((2, 2)),
            dma((2, chips)), dma((2, chips)), dma((2, chips)), dma((2, chips)),
            dma((n,)), dma((n,)), dma((n,)), dma((n,)), dma((n,)), dma((n,)), dma((n,)), dma((n,)), dma((n,)), dma((n,)),
            dma((2, 2, 2)), dma((2, 2, 2)), dma((2,)), dma((2, 2)),
            pltpu.SemaphoreType.REGULAR((2,)), pltpu.SemaphoreType.REGULAR((2,)),
        ],
        compiler_params=pltpu.CompilerParams(
            collective_id=0, has_side_effects=True, vmem_limit_bytes=67000000),
        name="head",
    )(x, gain, bias, w, aux)


def pass_kernel(x_ref, y_ref):
    y_ref[...] = x_ref[...]


def passed(x):
    rows, cols = x.shape
    size = row_chunk(rows, 128)
    spec = pl.BlockSpec((size, cols), lambda i: (i, 0))
    return pl.pallas_call(
        pass_kernel,
        grid=(rows // size,),
        out_shape=jax.ShapeDtypeStruct(x.shape, x.dtype),
        in_specs=[spec],
        out_specs=spec,
        name="passed",
    )(x)


def solution(mesh):
    n = mesh.shape["vp"]

    def per_device(hidden, norm_gain, norm_bias, w_blk, labels, loss_mask):
        seq, batch, depth = hidden.shape
        tokens = seq * batch
        aux = jnp.stack(
            [labels.astype(F32).reshape(2, tokens // 2), loss_mask.reshape(2, tokens // 2)], axis=1)
        dx, dw, dgain, dbias, loss, _ = head_call(
            n, hidden.reshape(2, tokens // 2, depth), norm_gain, norm_bias, w_blk, aux)
        return loss[0, :1], dx.reshape(seq, batch, depth), passed(dw), dgain, dbias

    tok_spec = P("vp", "dp")
    return jax.shard_map(
        per_device,
        mesh=mesh,
        in_specs=(P("vp", "dp", None), P(None), P(None), P(None, "vp"), tok_spec, tok_spec),
        out_specs=(P("dp"), P("vp", "dp", None), P("dp", "vp"), P("dp"), P("dp")),
        check_vma=False,
    )
```
